32 devices in a mesh: groups: 2 (over x), expert: 16 (over z, y, core).
Axes of the slice: x: 2, y: 2, z: 4, core: 2. Of those that a mesh axis runs over, the one named last changes fastest.
Arguments:
- tokens: bfloat16 [1024, 2048], P(('groups', 'expert')), parts along dimension 0, may hold values from -6 to 6
- expert_ids: int32 [1024, 2], P(('groups', 'expert')), parts along dimension 0, may hold values from 0 to 7, all different within a row; in each aligned block of 32 rows (0 to 31, 32 to 63, ...) at most 16 rows name the same one
- member_ids: int32 [1024], P(('groups', 'expert')), parts along dimension 0, may hold values from 0 to 7
- combine_weights: float32 [1024, 2], P(('groups', 'expert')), parts along dimension 0, may hold values from 0.25 to 1
- gate_weight: bfloat16 [2048, 57344], P(None, 'expert'), may hold values from -0.125 to 0.125
- up_weight: bfloat16 [2048, 57344], P(None, 'expert'), may hold values from -0.125 to 0.125
- down_weight: bfloat16 [57344, 2048], P('expert'), may hold values from -0.0625 to 0.0625
- input_factors: float32 [8, 8, 4096], replicated, may hold values from 0.5 to 2
- hidden_factors: float32 [8, 2, 57344], P(None, None, 'expert'), may hold values from 0.5 to 2
- output_factors: float32 [8, 8, 2048], replicated, may hold values from 0.5 to 2
Outputs:
- mixed: bfloat16 [1024, 2048], P(('groups', 'expert')), parts along dimension 0
The draws below stay inside these ranges and needn't reach their ends.
There are 2 independent parts, one for each index of `groups`. The reference program is written for one: setup_inputs(seed, part) draws one part's arguments, and reference() takes and returns one part's arrays. A program takes and returns all parts, laid end to end along the dimension named above; an argument that names none is the same for every part. Nothing has to cross between parts.
Inputs may be any that keep to these rules, and one draw needn't show every extreme that they name: `expert_ids`: the two experts of a token differ. Among the 32 tokens of one device no expert is named more than 16 times.
All inputs are finite; a program needn't handle non-finite values.
Results may differ from the reference program's by a relative error of at most 0.012.
Values may be sent and summed in bfloat16 or wider, within the bound.
A program may use at most 128 MiB of HBM per device.

```python
import math
import jax
import jax.numpy as jnp
import numpy as np
from jax import lax

D = 2048
FF = 7168
EXPERTS = 8
MEMBERS = 8
TOK_DEV = 32
CAP = 16
SPLIT = 2
FF_DEV = 3584
TOKENS = 512


def set_ends(entries, stream_key, smallest, top_value):
    longest = entries.shape.index(max(entries.shape))
    spots = []
    for shift in (0, 1):
        where = [jax.random.randint(jax.random.fold_in(stream_key, axis), (), 0, length) for axis, length in enumerate(entries.shape)]
        where[longest] = (where[longest] + shift) % entries.shape[longest]
        spots.append(tuple(where))
    return entries.at[spots[0]].set(smallest).at[spots[1]].set(top_value)


def steps_of(key, shape, cuts, low, largest):
    def one(position, blocks):
        heights = jax.random.uniform(jax.random.fold_in(jax.random.fold_in(key, 6), position), (blocks,), jnp.float32, low / len(cuts), largest / len(cuts))
        return jnp.repeat(jnp.exp(heights), shape[position] // blocks).reshape((-1,) + (1,) * (len(shape) - position - 1))

    factor_of = one(*cuts[0])
    for cut in cuts[1:]:
        factor_of = factor_of * one(*cut)
    return factor_of


def deal_out(stream_key, own, number, rows, amount, top, bound, slope):
    order = jax.random.permutation(stream_key, amount)
    crowded, usual = load_shares(amount, rows * top, bound, slope, True), load_shares(amount, rows * top, bound, slope, False)
    places = jnp.arange(amount)

    def named(tallies, turn):
        used = int((tallies > 0).sum())
        fixed = max(1, used // 4)
        moved = fixed + (places - fixed + turn * (used - fixed)) % max(1, amount - fixed)
        return jnp.zeros((amount,), jnp.int32).at[order[jnp.where(places < fixed, places, moved)]].set(jnp.asarray(tallies, jnp.int32))

    tallies = jnp.where(number % 4 == 0, named(crowded, number // 4), named(usual, number - number // 4 - 1))
    mixed = jax.random.permutation(jax.random.fold_in(own, 3), amount)
    donor, receiver = mixed[0:amount // 2 * 2:2], mixed[1:amount // 2 * 2:2]
    room = jnp.minimum(tallies[donor] - 1, bound - tallies[receiver]) // 2
    room = jnp.where((donor == order[0]) | (receiver == order[0]) | (tallies[receiver] == 0), 0, jnp.maximum(room, 0))
    moved = jax.random.randint(jax.random.fold_in(own, 4), (amount // 2,), 0, 1 << 20) % (room + 1)
    tallies = tallies.at[donor].add(-moved).at[receiver].add(moved)
    items = jnp.searchsorted(jnp.cumsum(tallies), jnp.arange(rows * top), side="right").astype(jnp.int32)
    grid = items.reshape(top, rows).T
    grid = grid[jax.random.permutation(jax.random.fold_in(own, 1), rows)]
    turn = jax.random.randint(jax.random.fold_in(own, 2), (rows, 1), 0, top)
    return jnp.take_along_axis(grid, (jnp.arange(top)[None, :] + turn) % top, axis=1)


def load_shares(count, total, most, lean, full):
    portions = [(1 << 20) // math.isqrt(grade ** lean) + 1 for grade in range(1, count + 1)]
    largest = most if full else min(most, max(-(-total // count), total * portions[0] // sum(portions)))
    least = 1 if total - largest >= count - 1 else 0
    holding, spare = [largest] + [least] * (count - 1), total - largest - least * (count - 1)
    while spare > 0:
        movable = [i for i in range(1, count) if holding[i] < largest] or [i for i in range(1, count) if holding[i] < most]
        whole, left = sum([portions[i] for i in movable]), spare
        for i in movable:
            more = min(most - holding[i], max(1, left * portions[i] // whole), spare)
            holding[i] = holding[i] + more
            spare = spare - more
    return np.array(holding)


def gaussian(own_key, shape, deviation, reach, split=(), kind=jnp.bfloat16):
    values = jax.random.normal(own_key, shape, jnp.float32) * deviation
    if len(split) > 0:
        values = steps_of(own_key, shape, split, -0.22, 0.18) * values
    return jnp.clip(values, min=-reach, max=reach).astype(kind)


def setup_inputs(seed: int = 0, part: int = 0) -> dict:
    keys = jax.random.split(jax.random.key(seed), 11)
    part_keys = jax.random.split(jax.random.fold_in(keys[10], part), 11)
    tokens = gaussian(part_keys[0], (TOKENS, D), 1.0, 6.0, ((0, 16),))
    expert_ids_keys = jax.random.split(jax.random.fold_in(part_keys[1], 1), TOKENS // TOK_DEV)
    expert_ids_turns = jax.random.permutation(jax.random.fold_in(part_keys[1], 3), TOKENS // TOK_DEV)
    expert_ids = jax.vmap(lambda own, number: deal_out(jax.random.fold_in(part_keys[1], 2), own, number, TOK_DEV, EXPERTS, 2, CAP, 2))(expert_ids_keys, expert_ids_turns).reshape((TOKENS, 2))
    member_ids = set_ends(jax.random.randint(part_keys[2], (TOKENS,), 0, MEMBERS), jax.random.fold_in(part_keys[2], 1), 0, MEMBERS - 1).astype(jnp.int32)
    combine_weights = jnp.clip(0.25 + 0.75 * jax.random.uniform(part_keys[3], (TOKENS, 2), jnp.float32) ** steps_of(part_keys[3], (TOKENS, 2), ((0, 16),), -0.2, 0.2), 0.25, 1.0)
    gate_weight = gaussian(keys[4], (D, EXPERTS * FF), D ** -0.5, 0.125, ((1, 16),))
    up_weight = gaussian(keys[5], (D, EXPERTS * FF), D ** -0.5, 0.125, ((1, 16),))
    down_weight = gaussian(keys[6], (EXPERTS * FF, D), FF ** -0.5, 0.0625, ((0, 16),))
    input_factors = jnp.clip(jnp.exp(jax.random.uniform(keys[7], (EXPERTS, MEMBERS, 2 * D), jnp.float32, math.log(0.5), math.log(2.0))), 0.5, 2.0)
    hidden_factors = jnp.clip(jnp.exp(math.log(2.0) - 1.3862944 * jax.random.uniform(keys[8], (MEMBERS, 2, EXPERTS * FF), jnp.float32) ** steps_of(keys[8], (MEMBERS, 2, EXPERTS * FF), ((2, 16),), -0.2, 0.2)), 0.5, 2.0)
    output_factors = jnp.clip(jnp.exp(jax.random.uniform(keys[9], (EXPERTS, MEMBERS, D), jnp.float32, math.log(0.5), math.log(2.0))), 0.5, 2.0)
    return {"tokens": tokens, "expert_ids": expert_ids, "member_ids": member_ids, "combine_weights": combine_weights, "gate_weight": gate_weight, "up_weight": up_weight, "down_weight": down_weight, "input_factors": input_factors, "hidden_factors": hidden_factors, "output_factors": output_factors}


def reference(tokens, expert_ids, member_ids, combine_weights, gate_weight, up_weight, down_weight, input_factors, hidden_factors, output_factors):
    pair_total = TOKENS * 2
    flat_expert = expert_ids.reshape(-1).astype(jnp.int32)
    ranking = jnp.argsort(flat_expert, stable=True).astype(jnp.int32)
    hits = (flat_expert[:, None] == jnp.arange(EXPERTS, dtype=jnp.int32)[None, :]).astype(jnp.int32)
    counts = jnp.sum(hits, 0).astype(jnp.int32)
    starts = (jnp.cumsum(counts) - counts).astype(jnp.int32)
    flat_weight = combine_weights.reshape(-1)
    block_rows = min(128, pair_total)
    total = jnp.zeros((TOKENS, D), jnp.float32)
    for expert_index in range(EXPERTS):
        low = expert_index * FF
        high = (expert_index + 1) * FF
        gate_cols = gate_weight[:, low:high]
        up_cols = up_weight[:, low:high]
        down_rows = down_weight[low:high].astype(jnp.float32).reshape(SPLIT, FF_DEV, D)
        in_table = input_factors[expert_index]
        out_table = output_factors[expert_index]
        first = starts[expert_index]
        number = counts[expert_index]

        def one_block(step_index, acc):
            local = step_index * block_rows + jnp.arange(block_rows, dtype=jnp.int32)
            valid = local < number
            picked = ranking[jnp.clip(first + local, 0, pair_total - 1)]
            token_index = picked // 2
            member = member_ids[token_index]
            row_data = tokens[token_index]
            in_scale = in_table[member]
            gate_in = (row_data * in_scale[:, :D]).astype(jnp.bfloat16)
            up_in = (row_data * in_scale[:, D:]).astype(jnp.bfloat16)
            gate = jnp.dot(gate_in, gate_cols, preferred_element_type=jnp.float32) * hidden_factors[member, 0, low:high]
            up = jnp.dot(up_in, up_cols, preferred_element_type=jnp.float32) * hidden_factors[member, 1, low:high]
            hidden = (jax.nn.silu(gate) * up).astype(jnp.bfloat16)
            pieces = jnp.einsum("rsf,sfd->rsd", hidden.astype(jnp.float32).reshape(block_rows, SPLIT, FF_DEV), down_rows)
            pieces = pieces.astype(jnp.bfloat16)
            result = jnp.sum(pieces.astype(jnp.float32), 1) * out_table[member]
            scale = jnp.where(valid, flat_weight[picked], jnp.zeros((), flat_weight.dtype))
            return acc.at[token_index].add(scale[:, None] * result)

        block_count = (number + block_rows - 1) // block_rows
        total = lax.fori_loop(jnp.zeros((), jnp.int32), block_count, one_block, total)
    return total.astype(jnp.bfloat16)
```

```python
import functools

import jax
import jax.numpy as jnp
from jax import lax
from jax.experimental import pallas as pl
from jax.experimental.pallas import tpu as pltpu
from jax.sharding import PartitionSpec as P

EXPERTS = 8
CAP = 16
LANES = 128
VMEM_LIMIT = 63 * 1024 * 1024
BATCHES = ((0, 1, 4, 6), (2, 3, 5, 7))
SEND_ORDER = (4, 6, 1, 2, 3, 5, 7)
PLACE = {k: (b, i) for b, ks in enumerate(BATCHES) for i, k in enumerate(ks)}
BF16 = jnp.bfloat16
F32 = jnp.float32


def tile_of(size):
    for tile in (512, 256, 128):
        if size % tile == 0:
            return tile
    return size


def parts_of(table):
    high = table.astype(BF16).astype(F32)
    rest = table - high
    mid = rest.astype(BF16).astype(F32)
    low = (rest - mid).astype(BF16).astype(F32)
    return high, mid, low


def pick(table, members):
    reps = table.shape[1] // LANES
    rows = []
    for which in members:
        full = jnp.concatenate([which] * reps, axis=1)
        rows.append(jnp.take_along_axis(table, full, axis=0, mode="promise_in_bounds"))
    return jnp.concatenate(rows, axis=0)


def kernel(
    n,
    ids_hbm,
    mem_hbm,
    cw_hbm,
    tok_hbm,
    hidf_hbm,
    wg_hbm,
    wu_hbm,
    wd_hbm,
    inf_hbm,
    outf_hbm,
    o_ref,
    ids_ref,
    mem_ref,
    cw_ref,
    tok_ref,
    hidf_ref,
    wg,
    wu,
    wd,
    inf,
    outf,
    tab_hid,
    send,
    recv,
    who,
    weigh,
    gate_in,
    up_in,
    hidden,
    psend,
    precv,
    osend,
    home,
    placing,
    wsem,
    fsem,
    dsend,
    drecv,
    psems,
    precs,
    hsend,
    hrecv,
    xsend,
    xrecv,
):
    split = n // EXPERTS
    toks, width = tok_ref.shape
    units = wg.shape[1]
    seg = EXPERTS * CAP
    me = lax.axis_index("expert")
    own = lax.div(me, split)
    part = lax.rem(me, split)
    wide = tile_of(width)
    tile = tile_of(units)
    unit_tiles = units // tile
    tiles, _, out_tile = home.shape
    batch_rows = recv.shape[0] // len(BATCHES)
    share_rows = batch_rows // split

    def expert_at(k):
        return lax.bitwise_xor(own, k)

    def part_at(j):
        return lax.rem(part + (j + split) % split, split)

    def far(k):
        return {"expert": expert_at(k) * split + part}

    def near(j):
        return {"expert": own * split + part_at(j)}

    def rows(index, count=CAP):
        return pl.ds(pl.multiple_of(index * count, count), count)

    barrier = pltpu.get_barrier_semaphore()
    for k in range(1, EXPERTS):
        pl.semaphore_signal(barrier, inc=1, device_id=far(k), device_id_type=pl.DeviceIdType.MESH)
    for j in range(1, split):
        pl.semaphore_signal(barrier, inc=1, device_id=near(j), device_id_type=pl.DeviceIdType.MESH)

    small = [
        pltpu.make_async_copy(src, dst, fsem.at[i])
        for i, (src, dst) in enumerate(
            ((ids_hbm, ids_ref), (mem_hbm, mem_ref), (cw_hbm, cw_ref), (tok_hbm, tok_ref))
        )
    ]
    loads = [
        pltpu.make_async_copy(inf_hbm.at[own], inf, fsem.at[4]),
        pltpu.make_async_copy(hidf_hbm, hidf_ref, fsem.at[5]),
        pltpu.make_async_copy(outf_hbm.at[own], outf, fsem.at[6]),
    ]

    def column_load(src, dst, size, t, sem):
        cols = pl.ds(t * size, size)
        return pltpu.make_async_copy(src.at[:, cols], dst.at[:, cols], sem)

    first = [
        [
            column_load(wg_hbm, wg, tile, t, wsem.at[0, t]),
            column_load(wu_hbm, wu, tile, t, wsem.at[1, t]),
        ]
        for t in range(unit_tiles)
    ]
    second = [column_load(wd_hbm, wd, out_tile, t, wsem.at[2, t]) for t in range(tiles)]
    for copy in small + loads:
        copy.start()
    for copy in sum(first, []) + second:
        copy.start(priority=1)

    down_i = lax.broadcasted_iota(jnp.int32, (toks, toks), 0)
    across = lax.broadcasted_iota(jnp.int32, (toks, toks), 1)

    def column(row):
        spread = jnp.broadcast_to(row.astype(F32), (toks, toks))
        return jnp.sum(jnp.where(across == down_i, spread, 0.0), axis=1, keepdims=True)

    lane = lax.broadcasted_iota(jnp.int32, (toks, seg), 1)
    lane_expert = lax.shift_right_logical(lane, CAP.bit_length() - 1)
    lane_slot = lax.bitwise_and(lane, CAP - 1)
    for copy in small[:3]:
        copy.wait()
    hit0 = column(ids_ref[0:1, :]) == lane_expert.astype(F32)
    hit1 = column(ids_ref[1:2, :]) == lane_expert.astype(F32)
    named = jnp.where(hit0 | hit1, 1.0, 0.0)
    earlier = jnp.where(across < down_i, 1.0, 0.0)
    rank = jnp.dot(earlier.astype(BF16), named.astype(BF16), preferred_element_type=F32)
    placed = jnp.where(rank == lane_slot.astype(F32), named, 0.0)
    placing[...] = placed.astype(BF16)
    member = column(mem_ref[...])
    col = lax.broadcasted_iota(jnp.int32, (toks, LANES), 1)

    def gather(which, data):
        return lax.dot_general(
            which.astype(BF16), data.astype(BF16), (((0,), (0,)), ((), ())), preferred_element_type=F32
        )

    meta_rows = jnp.zeros((seg, LANES), F32)
    for route, hit in ((0, hit0), (1, hit1)):
        meta = jnp.where(col == 0, member, 0.0)
        for spot, piece in enumerate(parts_of(column(cw_ref[route : route + 1, :]))):
            meta = jnp.where(col == 1 + spot, piece, meta)
        meta_rows = meta_rows + gather(jnp.where(hit, placed, 0.0), meta)
    send[:, width:] = meta_rows.astype(BF16)
    small[3].wait()
    for t in range(width // wide):
        cols = slice(t * wide, (t + 1) * wide)
        send[:, cols] = gather(placed, tok_ref[:, cols]).astype(BF16)

    pl.semaphore_wait(barrier, EXPERTS - 1 + split - 1)

    def landed(k, j):
        batch, slot = PLACE[k]
        each = len(BATCHES[batch])
        return rows(batch * split * each + part_at(-j) * each + slot)

    def direct(k):
        return pltpu.make_async_remote_copy(
            src_ref=send.at[rows(expert_at(k))],
            dst_ref=recv.at[landed(k, 0)],
            send_sem=dsend.at[k],
            recv_sem=drecv.at[k],
            device_id=far(k),
            device_id_type=pl.DeviceIdType.MESH,
        )

    def handed(k, j):
        return pltpu.make_async_remote_copy(
            src_ref=recv.at[landed(k, 0)] if k else send.at[rows(own)],
            dst_ref=recv.at[landed(k, 0)],
            send_sem=xsend.at[k, j],
            recv_sem=xrecv.at[k, j],
            device_id=near(j),
            device_id_type=pl.DeviceIdType.MESH,
        )

    for k in SEND_ORDER:
        direct(k).start()
    for j in range(1, split):
        handed(0, j).start()
    recv[landed(0, 0), :] = send[rows(own), :]

    for copy in loads:
        copy.wait()
    for g in range(2):
        for t in range(unit_tiles):
            cols = slice(t * tile, (t + 1) * tile)
            tab_hid[g, :, cols] = hidf_ref[:, g, cols]

    def hand_on(k):
        pltpu.make_async_remote_copy(
            src_ref=recv.at[landed(k, 0)],
            dst_ref=recv.at[landed(k, 0)],
            send_sem=dsend.at[k],
            recv_sem=drecv.at[k],
            device_id=far(k),
            device_id_type=pl.DeviceIdType.MESH,
        ).wait_recv()
        for j in range(1, split):
            handed(k, j).start()

    def got(k, j):
        pltpu.make_async_remote_copy(
            src_ref=recv.at[landed(k, j)],
            dst_ref=recv.at[landed(k, j)],
            send_sem=xsend.at[k, j],
            recv_sem=xrecv.at[k, j],
            device_id=near(j),
            device_id_type=pl.DeviceIdType.MESH,
        ).wait_recv()

    def scale_unit(k, j):
        mine = landed(k, j)
        meta = recv[mine, width:].astype(F32)
        which = jnp.broadcast_to(meta[:, 0:1], (CAP, LANES)).astype(jnp.int32)
        who[mine, :] = which
        if j == 0:
            batch, slot = PLACE[k]
            spot = lax.broadcasted_iota(jnp.int32, (CAP, LANES), 1)
            weight = jnp.sum(
                jnp.where((spot >= 1) & (spot < 4), meta, 0.0), axis=1, keepdims=True
            )
            weigh[batch, slot * CAP : (slot + 1) * CAP, :] = jnp.broadcast_to(weight, (CAP, LANES))
        members = [which[r : r + 8] for r in range(0, CAP, 8)]
        for t in range(width // wide):
            cols = slice(t * wide, (t + 1) * wide)
            data = recv[mine, cols].astype(F32)
            gate_in[mine, cols] = (data * pick(inf[:, cols], members)).astype(BF16)
            cols_up = slice(width + t * wide, width + (t + 1) * wide)
            up_in[mine, cols] = (data * pick(inf[:, cols_up], members)).astype(BF16)

    def hidden_units(b, low, high):
        mine = slice(b * batch_rows, (b + 1) * batch_rows)

        def hidden_tile(t, carry):
            cols = pl.ds(pl.multiple_of(t * tile, tile), tile)
            members = [
                who[b * batch_rows + r : b * batch_rows + r + 8, :] for r in range(0, batch_rows, 8)
            ]
            gate = jnp.dot(gate_in[mine, :], wg[:, cols], preferred_element_type=F32)
            gate = gate * pick(tab_hid[0, :, cols], members)
            up = jnp.dot(up_in[mine, :], wu[:, cols], preferred_element_type=F32)
            up = up * pick(tab_hid[1, :, cols], members)
            hidden[:, cols] = (gate / (1.0 + jnp.exp(-gate)) * up).astype(BF16)
            return carry

        lax.fori_loop(low, high, hidden_tile, 0, unroll=high - low)

    def share(b, t, j):
        return pltpu.make_async_remote_copy(
            src_ref=psend.at[b, t, rows(part_at(j), share_rows)],
            dst_ref=precv.at[b, t, j],
            send_sem=psems.at[b, t, j],
            recv_sem=precs.at[b, t, j],
            device_id=near(j),
            device_id_type=pl.DeviceIdType.MESH,
        )

    def back(t, k):
        batch, slot = PLACE[k]
        return pltpu.make_async_remote_copy(
            src_ref=osend.at[batch, t, pl.ds(slot * CAP, CAP)],
            dst_ref=home.at[t, rows(own)],
            send_sem=hsend.at[t, k],
            recv_sem=hrecv.at[t, k],
            device_id=far(k),
            device_id_type=pl.DeviceIdType.MESH,
        )

    def down_tile(b, t):
        cols = slice(t * out_tile, (t + 1) * out_tile)
        psend[b, t] = jnp.dot(hidden[...], wd[:, cols], preferred_element_type=F32).astype(BF16)
        for j in range(1, split):
            share(b, t, j).start()

    def finish(b, t):
        base = b * batch_rows + part * share_rows
        members = [
            who[pl.ds(pl.multiple_of(base + r, 8), 8), :] for r in range(0, share_rows, 8)
        ]
        total = psend[b, t, rows(part, share_rows), :].astype(F32)
        for j in range(1, split):
            share(b, t, j).wait_recv()
            total = total + precv[b, t, j].astype(F32)
        cols = slice(t * out_tile, (t + 1) * out_tile)
        weight = jnp.concatenate([weigh[b]] * (out_tile // LANES), axis=1)
        value = (total * pick(outf[:, cols], members) * weight).astype(BF16)
        osend[b, t] = value
        for slot, k in enumerate(BATCHES[b]):
            if k:
                back(t, k).start()
            else:
                home[t, rows(own), :] = value[slot * CAP : (slot + 1) * CAP]

    half = (unit_tiles + 1) // 2
    ahead = max(0, tiles - 2)

    scale_unit(0, 0)
    for k in BATCHES[0][1:]:
        hand_on(k)
        scale_unit(k, 0)
    for k in BATCHES[0]:
        for j in range(1, split):
            got(k, j)
            scale_unit(k, j)
    for copies in first[:half]:
        for copy in copies:
            copy.wait()
    hidden_units(0, 0, half)
    for copies in first[half:]:
        for copy in copies:
            copy.wait()
    for k in BATCHES[1][:2]:
        hand_on(k)
    hidden_units(0, half, unit_tiles)
    hand_on(BATCHES[1][2])
    for t in range(tiles):
        second[t].wait()
        down_tile(0, t)
        if t >= 2:
            finish(0, t - 2)
    hand_on(BATCHES[1][3])
    for k in BATCHES[1]:
        scale_unit(k, 0)
    for t in range(ahead, tiles):
        finish(0, t)
    for k in BATCHES[1]:
        for j in range(1, split):
            got(k, j)
            scale_unit(k, j)
    hidden_units(1, 0, unit_tiles)
    for t in range(tiles):
        down_tile(1, t)
        if t >= 2:
            finish(1, t - 2)
    for t in range(ahead, tiles):
        finish(1, t)

    for t in range(tiles):
        cols = slice(t * out_tile, (t + 1) * out_tile)
        for k in range(1, EXPERTS):
            back(t, k).wait_recv()
        o_ref[:, cols] = jnp.dot(placing[...], home[t], preferred_element_type=F32).astype(BF16)

    for k in range(1, EXPERTS):
        direct(k).wait_send()
    for k in range(EXPERTS):
        for j in range(1, split):
            handed(k, j).wait_send()
    for t in range(tiles):
        for b in range(len(BATCHES)):
            for j in range(1, split):
                share(b, t, j).wait_send()
        for k in range(1, EXPERTS):
            back(t, k).wait_send()


def per_device(
    tokens,
    expert_ids,
    member_ids,
    combine_weights,
    gate_weight,
    up_weight,
    down_weight,
    input_factors,
    hidden_factors,
    output_factors,
):
    n = lax.axis_size("expert")
    split = n // EXPERTS
    toks, width = tokens.shape
    units = gate_weight.shape[1]
    members = input_factors.shape[1]
    seg = EXPERTS * CAP
    all_rows = n * CAP
    batches = len(BATCHES)
    batch_rows = all_rows // batches
    out_tile = tile_of(width)
    tiles = width // out_tile
    unit_tiles = units // tile_of(units)
    vmem = pl.BlockSpec(memory_space=pltpu.VMEM)
    hbm = pl.BlockSpec(memory_space=pl.ANY)
    dma = pltpu.SemaphoreType.DMA
    return pl.pallas_call(
        functools.partial(kernel, n),
        out_shape=pltpu.VMEM((toks, width), BF16),
        in_specs=[hbm] * 10,
        out_specs=vmem,
        scratch_shapes=[
            pltpu.VMEM((2, toks), jnp.int32),
            pltpu.VMEM((1, toks), jnp.int32),
            pltpu.VMEM((2, toks), F32),
            pltpu.VMEM((toks, width), BF16),
            pltpu.VMEM(hidden_factors.shape, F32),
            pltpu.VMEM((width, units), BF16),
            pltpu.VMEM((width, units), BF16),
            pltpu.VMEM((units, width), BF16),
            pltpu.VMEM((members, 2 * width), F32),
            pltpu.VMEM((members, width), F32),
            pltpu.VMEM((2, members, units), F32),
            pltpu.VMEM((seg, width + LANES), BF16),
            pltpu.VMEM((all_rows, width + LANES), BF16),
            pltpu.VMEM((all_rows, LANES), jnp.int32),
            pltpu.VMEM((batches, seg // batches, LANES), F32),
            pltpu.VMEM((all_rows, width), BF16),
            pltpu.VMEM((all_rows, width), BF16),
            pltpu.VMEM((batch_rows, units), BF16),
            pltpu.VMEM((batches, tiles, batch_rows, out_tile), BF16),
            pltpu.VMEM((batches, tiles, split, seg // batches, out_tile), BF16),
            pltpu.VMEM((batches, tiles, seg // batches, out_tile), BF16),
            pltpu.VMEM((tiles, seg, out_tile), BF16),
            pltpu.VMEM((toks, seg), BF16),
            dma((3, max(unit_tiles, tiles))),
            dma((7,)),
            dma((EXPERTS,)),
            dma((EXPERTS,)),
            dma((batches, tiles, split)),
            dma((batches, tiles, split)),
            dma((tiles, EXPERTS)),
            dma((tiles, EXPERTS)),
            dma((EXPERTS, split)),
            dma((EXPERTS, split)),
        ],
        compiler_params=pltpu.CompilerParams(
            collective_id=0, has_side_effects=True, vmem_limit_bytes=VMEM_LIMIT
        ),
        name="moe_step",
    )(
        expert_ids.T,
        member_ids.reshape(1, toks),
        combine_weights.T,
        tokens,
        hidden_factors,
        gate_weight,
        up_weight,
        down_weight,
        input_factors,
        output_factors,
    )


def solution(mesh):
    in_specs = (
        P(("groups", "expert"), None),
        P(("groups", "expert"), None),
        P(("groups", "expert")),
        P(("groups", "expert"), None),
        P(None, "expert"),
        P(None, "expert"),
        P("expert", None),
        P(),
        P(None, None, "expert"),
        P(),
    )
    out_specs = P(("groups", "expert"), None)
    return jax.shard_map(
        per_device, mesh=mesh, in_specs=in_specs, out_specs=out_specs, check_vma=False
    )
```

```python
import functools

import jax
import jax.numpy as jnp
from jax import lax
from jax.experimental import pallas as pl
from jax.experimental.pallas import tpu as pltpu
from jax.sharding import PartitionSpec as P

EXPERTS = 8
CAP = 16
LANES = 128
VMEM_LIMIT = 63 * 1024 * 1024
BATCHES = ((0, 1, 4, 6), (2, 3, 5, 7))
LAG = 2
SEND_ORDER = (4, 6, 1, 2, 3)
LATER = (5, 7)
GROUPS = (2, 4)
RETURNS = ((1, 4, 6), (2, 3, 5, 7))
PLACE = {k: (b, i) for b, ks in enumerate(BATCHES) for i, k in enumerate(ks)}
BF16 = jnp.bfloat16
F32 = jnp.float32


def tile_of(size):
    for tile in (512, 256, 128):
        if size % tile == 0:
            return tile
    return size


def parts_of(table):
    high = table.astype(BF16).astype(F32)
    rest = table - high
    mid = rest.astype(BF16).astype(F32)
    low = (rest - mid).astype(BF16).astype(F32)
    return high, mid, low


def pick(table, members):
    reps = table.shape[1] // LANES
    rows = []
    for which in members:
        full = jnp.concatenate([which] * reps, axis=1)
        rows.append(jnp.take_along_axis(table, full, axis=0, mode="promise_in_bounds"))
    return jnp.concatenate(rows, axis=0)


def kernel(
    n,
    ids_hbm,
    mem_hbm,
    cw_hbm,
    tok_hbm,
    hidf_hbm,
    wg_hbm,
    wu_hbm,
    wd_hbm,
    inf_hbm,
    outf_hbm,
    o_ref,
    ids_ref,
    mem_ref,
    cw_ref,
    tok_ref,
    hidf_ref,
    wg,
    wu,
    wd,
    inf,
    outf,
    tab_hid,
    send,
    recv,
    who,
    weigh,
    gate_in,
    up_in,
    hidden,
    psend,
    precv,
    osend,
    home,
    placing,
    wsem,
    fsem,
    dsend,
    drecv,
    psems,
    precs,
    hsend,
    hrecv,
    xsend,
    xrecv,
):
    split = n // EXPERTS
    toks, width = tok_ref.shape
    units = wg.shape[1]
    seg = EXPERTS * CAP
    me = lax.axis_index("expert")
    own = lax.div(me, split)
    part = lax.rem(me, split)
    wide = tile_of(width)
    tile = tile_of(units)
    unit_tiles = units // tile
    out_tile = tile_of(width)
    tiles = width // out_tile
    ends = [[tiles * (g + 1) // n_g for g in range(n_g)] for n_g in GROUPS]
    batch_rows = recv.shape[0] // len(BATCHES)
    share_rows = batch_rows // split

    def expert_at(k):
        return lax.bitwise_xor(own, k)

    def part_at(j):
        return lax.rem(part + (j + split) % split, split)

    def far(k):
        return {"expert": expert_at(k) * split + part}

    def near(j):
        return {"expert": own * split + part_at(j)}

    def rows(index, count=CAP):
        return pl.ds(pl.multiple_of(index * count, count), count)

    barrier = pltpu.get_barrier_semaphore()
    for k in range(1, EXPERTS):
        pl.semaphore_signal(barrier, inc=1, device_id=far(k), device_id_type=pl.DeviceIdType.MESH)
    for j in range(1, split):
        pl.semaphore_signal(barrier, inc=1, device_id=near(j), device_id_type=pl.DeviceIdType.MESH)

    small = [
        pltpu.make_async_copy(src, dst, fsem.at[i])
        for i, (src, dst) in enumerate(
            ((ids_hbm, ids_ref), (mem_hbm, mem_ref), (cw_hbm, cw_ref), (tok_hbm, tok_ref))
        )
    ]
    loads = [
        pltpu.make_async_copy(inf_hbm.at[own], inf, fsem.at[4]),
        pltpu.make_async_copy(hidf_hbm, hidf_ref, fsem.at[5]),
        pltpu.make_async_copy(outf_hbm.at[own], outf, fsem.at[6]),
    ]

    def column_load(src, dst, size, t, sem):
        cols = pl.ds(t * size, size)
        return pltpu.make_async_copy(src.at[:, cols], dst.at[:, cols], sem)

    first = [
        [
            column_load(wg_hbm, wg, tile, t, wsem.at[0, t]),
            column_load(wu_hbm, wu, tile, t, wsem.at[1, t]),
        ]
        for t in range(unit_tiles)
    ]
    second = [column_load(wd_hbm, wd, out_tile, t, wsem.at[2, t]) for t in range(tiles)]
    for copy in small + loads:
        copy.start()
    for copy in sum(first, []) + second:
        copy.start(priority=1)

    down_i = lax.broadcasted_iota(jnp.int32, (toks, toks), 0)
    across = lax.broadcasted_iota(jnp.int32, (toks, toks), 1)

    def column(row):
        spread = jnp.broadcast_to(row.astype(F32), (toks, toks))
        return jnp.sum(jnp.where(across == down_i, spread, 0.0), axis=1, keepdims=True)

    lane = lax.broadcasted_iota(jnp.int32, (toks, seg), 1)
    lane_expert = lax.shift_right_logical(lane, CAP.bit_length() - 1)
    lane_slot = lax.bitwise_and(lane, CAP - 1)
    for copy in small[:3]:
        copy.wait()
    hit0 = column(ids_ref[0:1, :]) == lane_expert.astype(F32)
    hit1 = column(ids_ref[1:2, :]) == lane_expert.astype(F32)
    named = jnp.where(hit0 | hit1, 1.0, 0.0)
    earlier = jnp.where(across < down_i, 1.0, 0.0)
    rank = jnp.dot(earlier.astype(BF16), named.astype(BF16), preferred_element_type=F32)
    placed = jnp.where(rank == lane_slot.astype(F32), named, 0.0)
    placing[...] = placed.astype(BF16)
    member = column(mem_ref[...])
    col = lax.broadcasted_iota(jnp.int32, (toks, LANES), 1)

    def gather(which, data):
        return lax.dot_general(
            which.astype(BF16), data.astype(BF16), (((0,), (0,)), ((), ())), preferred_element_type=F32
        )

    meta_rows = jnp.zeros((seg, LANES), F32)
    for route, hit in ((0, hit0), (1, hit1)):
        meta = jnp.where(col == 0, member, 0.0)
        for spot, piece in enumerate(parts_of(column(cw_ref[route : route + 1, :]))):
            meta = jnp.where(col == 1 + spot, piece, meta)
        meta_rows = meta_rows + gather(jnp.where(hit, placed, 0.0), meta)
    send[:, width:] = meta_rows.astype(BF16)
    small[3].wait()
    for t in range(width // wide):
        cols = slice(t * wide, (t + 1) * wide)
        send[:, cols] = gather(placed, tok_ref[:, cols]).astype(BF16)

    pl.semaphore_wait(barrier, EXPERTS - 1 + split - 1)

    def landed(k, j):
        batch, slot = PLACE[k]
        each = len(BATCHES[batch])
        return rows(batch * split * each + part_at(-j) * each + slot)

    def direct(k):
        return pltpu.make_async_remote_copy(
            src_ref=send.at[rows(expert_at(k))],
            dst_ref=recv.at[landed(k, 0)],
            send_sem=dsend.at[k],
            recv_sem=drecv.at[k],
            device_id=far(k),
            device_id_type=pl.DeviceIdType.MESH,
        )

    def handed(k, j):
        return pltpu.make_async_remote_copy(
            src_ref=recv.at[landed(k, 0)] if k else send.at[rows(own)],
            dst_ref=recv.at[landed(k, 0)],
            send_sem=xsend.at[k, j],
            recv_sem=xrecv.at[k, j],
            device_id=near(j),
            device_id_type=pl.DeviceIdType.MESH,
        )

    for k in SEND_ORDER:
        direct(k).start()
    for j in range(1, split):
        handed(0, j).start()
    recv[landed(0, 0), :] = send[rows(own), :]

    for copy in loads:
        copy.wait()
    for g in range(2):
        for t in range(unit_tiles):
            cols = slice(t * tile, (t + 1) * tile)
            tab_hid[g, :, cols] = hidf_ref[:, g, cols]

    def hand_on(k):
        pltpu.make_async_remote_copy(
            src_ref=recv.at[landed(k, 0)],
            dst_ref=recv.at[landed(k, 0)],
            send_sem=dsend.at[k],
            recv_sem=drecv.at[k],
            device_id=far(k),
            device_id_type=pl.DeviceIdType.MESH,
        ).wait_recv()
        for j in range(1, split):
            handed(k, j).start()

    def got(k, j):
        pltpu.make_async_remote_copy(
            src_ref=recv.at[landed(k, j)],
            dst_ref=recv.at[landed(k, j)],
            send_sem=xsend.at[k, j],
            recv_sem=xrecv.at[k, j],
            device_id=near(j),
            device_id_type=pl.DeviceIdType.MESH,
        ).wait_recv()

    def scale_unit(k, j):
        mine = landed(k, j)
        meta = recv[mine, width:].astype(F32)
        which = jnp.broadcast_to(meta[:, 0:1], (CAP, LANES)).astype(jnp.int32)
        who[mine, :] = which
        if j == 0:
            batch, slot = PLACE[k]
            spot = lax.broadcasted_iota(jnp.int32, (CAP, LANES), 1)
            weight = jnp.sum(
                jnp.where((spot >= 1) & (spot < 4), meta, 0.0), axis=1, keepdims=True
            )
            weigh[batch, slot * CAP : (slot + 1) * CAP, :] = jnp.broadcast_to(weight, (CAP, LANES))
        members = [which[r : r + 8] for r in range(0, CAP, 8)]
        for t in range(width // wide):
            cols = slice(t * wide, (t + 1) * wide)
            data = recv[mine, cols].astype(F32)
            gate_in[mine, cols] = (data * pick(inf[:, cols], members)).astype(BF16)
            cols_up = slice(width + t * wide, width + (t + 1) * wide)
            up_in[mine, cols] = (data * pick(inf[:, cols_up], members)).astype(BF16)

    def hidden_units(b, low, high):
        mine = slice(b * batch_rows, (b + 1) * batch_rows)

        def hidden_tile(t, carry):
            cols = pl.ds(pl.multiple_of(t * tile, tile), tile)
            members = [
                who[b * batch_rows + r : b * batch_rows + r + 8, :] for r in range(0, batch_rows, 8)
            ]
            gate = jnp.dot(gate_in[mine, :], wg[:, cols], preferred_element_type=F32)
            gate = gate * pick(tab_hid[0, :, cols], members)
            up = jnp.dot(up_in[mine, :], wu[:, cols], preferred_element_type=F32)
            up = up * pick(tab_hid[1, :, cols], members)
            hidden[:, cols] = (gate / (1.0 + jnp.exp(-gate)) * up).astype(BF16)
            return carry

        lax.fori_loop(low, high, hidden_tile, 0, unroll=high - low)

    def share(b, t, j):
        return pltpu.make_async_remote_copy(
            src_ref=psend.at[b, t, rows(part_at(j), share_rows)],
            dst_ref=precv.at[b, t, j],
            send_sem=psems.at[b, t, j],
            recv_sem=precs.at[b, t, j],
            device_id=near(j),
            device_id_type=pl.DeviceIdType.MESH,
        )

    def back(g, k):
        batch, slot = PLACE[k]
        low = ends[batch][g - 1] if g else 0
        cols = pl.ds(low * out_tile, (ends[batch][g] - low) * out_tile)
        return pltpu.make_async_remote_copy(
            src_ref=osend.at[batch, pl.ds(slot * CAP, CAP), cols],
            dst_ref=home.at[rows(own), cols],
            send_sem=hsend.at[g, k],
            recv_sem=hrecv.at[g, k],
            device_id=far(k),
            device_id_type=pl.DeviceIdType.MESH,
        )

    def down_tile(b, t):
        cols = slice(t * out_tile, (t + 1) * out_tile)
        psend[b, t] = jnp.dot(hidden[...], wd[:, cols], preferred_element_type=F32).astype(BF16)
        for j in range(1, split):
            share(b, t, j).start()

    def finish(b, t):
        base = b * batch_rows + part * share_rows
        members = [
            who[pl.ds(pl.multiple_of(base + r, 8), 8), :] for r in range(0, share_rows, 8)
        ]
        total = psend[b, t, rows(part, share_rows), :].astype(F32)
        for j in range(1, split):
            share(b, t, j).wait_recv()
            total = total + precv[b, t, j].astype(F32)
        cols = slice(t * out_tile, (t + 1) * out_tile)
        weight = jnp.concatenate([weigh[b]] * (out_tile // LANES), axis=1)
        value = (total * pick(outf[:, cols], members) * weight).astype(BF16)
        osend[b, :, cols] = value
        if b == PLACE[0][0]:
            slot = PLACE[0][1]
            home[rows(own), cols] = value[slot * CAP : (slot + 1) * CAP]
        if t + 1 in ends[b]:
            for k in RETURNS[b]:
                back(ends[b].index(t + 1), k).start()

    half = (unit_tiles + 1) // 2
    ahead = max(0, tiles - LAG)

    scale_unit(0, 0)
    for k in BATCHES[0][1:]:
        hand_on(k)
        scale_unit(k, 0)
    for k in LATER:
        direct(k).start()
    for k in BATCHES[0]:
        for j in range(1, split):
            got(k, j)
            scale_unit(k, j)
    for copies in first[:half]:
        for copy in copies:
            copy.wait()
    hidden_units(0, 0, half)
    for copies in first[half:]:
        for copy in copies:
            copy.wait()
    for k in BATCHES[1][:2]:
        hand_on(k)
    hidden_units(0, half, unit_tiles)
    for t in range(tiles):
        second[t].wait()
        down_tile(0, t)
        if t >= LAG:
            finish(0, t - LAG)
        if t == min(2, tiles - 1):
            hand_on(BATCHES[1][2])
    hand_on(BATCHES[1][3])
    for k in BATCHES[1]:
        scale_unit(k, 0)
    for t in range(ahead, tiles):
        finish(0, t)
    for k in BATCHES[1]:
        for j in range(1, split):
            got(k, j)
            scale_unit(k, j)
    hidden_units(1, 0, unit_tiles)
    for t in range(tiles):
        down_tile(1, t)
        if t >= LAG:
            finish(1, t - LAG)
    for t in range(ahead, tiles):
        finish(1, t)

    for t in range(tiles):
        cols = slice(t * out_tile, (t + 1) * out_tile)
        for k in range(1, EXPERTS):
            stops = ends[PLACE[k][0]]
            for g, begin in enumerate([0] + stops[:-1]):
                if begin == t:
                    back(g, k).wait_recv()
        o_ref[:, cols] = jnp.dot(
            placing[...], home[:, cols], preferred_element_type=F32
        ).astype(BF16)

    for k in range(1, EXPERTS):
        direct(k).wait_send()
    for k in range(EXPERTS):
        for j in range(1, split):
            handed(k, j).wait_send()
    for t in range(tiles):
        for b in range(len(BATCHES)):
            for j in range(1, split):
                share(b, t, j).wait_send()
    for k in range(1, EXPERTS):
        for g in range(len(ends[PLACE[k][0]])):
            back(g, k).wait_send()


def per_device(
    tokens,
    expert_ids,
    member_ids,
    combine_weights,
    gate_weight,
    up_weight,
    down_weight,
    input_factors,
    hidden_factors,
    output_factors,
):
    n = lax.axis_size("expert")
    split = n // EXPERTS
    toks, width = tokens.shape
    units = gate_weight.shape[1]
    members = input_factors.shape[1]
    seg = EXPERTS * CAP
    all_rows = n * CAP
    batches = len(BATCHES)
    batch_rows = all_rows // batches
    out_tile = tile_of(width)
    tiles = width // out_tile
    unit_tiles = units // tile_of(units)
    vmem = pl.BlockSpec(memory_space=pltpu.VMEM)
    hbm = pl.BlockSpec(memory_space=pl.ANY)
    dma = pltpu.SemaphoreType.DMA
    return pl.pallas_call(
        functools.partial(kernel, n),
        out_shape=pltpu.VMEM((toks, width), BF16),
        in_specs=[hbm] * 10,
        out_specs=vmem,
        scratch_shapes=[
            pltpu.VMEM((2, toks), jnp.int32),
            pltpu.VMEM((1, toks), jnp.int32),
            pltpu.VMEM((2, toks), F32),
            pltpu.VMEM((toks, width), BF16),
            pltpu.VMEM(hidden_factors.shape, F32),
            pltpu.VMEM((width, units), BF16),
            pltpu.VMEM((width, units), BF16),
            pltpu.VMEM((units, width), BF16),
            pltpu.VMEM((members, 2 * width), F32),
            pltpu.VMEM((members, width), F32),
            pltpu.VMEM((2, members, units), F32),
            pltpu.VMEM((seg, width + LANES), BF16),
            pltpu.VMEM((all_rows, width + LANES), BF16),
            pltpu.VMEM((all_rows, LANES), jnp.int32),
            pltpu.VMEM((batches, seg // batches, LANES), F32),
            pltpu.VMEM((all_rows, width), BF16),
            pltpu.VMEM((all_rows, width), BF16),
            pltpu.VMEM((batch_rows, units), BF16),
            pltpu.VMEM((batches, tiles, batch_rows, out_tile), BF16),
            pltpu.VMEM((batches, tiles, split, seg // batches, out_tile), BF16),
            pltpu.VMEM((batches, seg // batches, width), BF16),
            pltpu.VMEM((seg, width), BF16),
            pltpu.VMEM((toks, seg), BF16),
            dma((3, max(unit_tiles, tiles))),
            dma((7,)),
            dma((EXPERTS,)),
            dma((EXPERTS,)),
            dma((batches, tiles, split)),
            dma((batches, tiles, split)),
            dma((tiles, EXPERTS)),
            dma((tiles, EXPERTS)),
            dma((EXPERTS, split)),
            dma((EXPERTS, split)),
        ],
        compiler_params=pltpu.CompilerParams(
            collective_id=0, has_side_effects=True, vmem_limit_bytes=VMEM_LIMIT
        ),
        name="moe_step",
    )(
        expert_ids.T,
        member_ids.reshape(1, toks),
        combine_weights.T,
        tokens,
        hidden_factors,
        gate_weight,
        up_weight,
        down_weight,
        input_factors,
        output_factors,
    )


def solution(mesh):
    in_specs = (
        P(("groups", "expert"), None),
        P(("groups", "expert"), None),
        P(("groups", "expert")),
        P(("groups", "expert"), None),
        P(None, "expert"),
        P(None, "expert"),
        P("expert", None),
        P(),
        P(None, None, "expert"),
        P(),
    )
    out_specs = P(("groups", "expert"), None)
    return jax.shard_map(
        per_device, mesh=mesh, in_specs=in_specs, out_specs=out_specs, check_vma=False
    )
```

```python
import functools

import jax
import jax.numpy as jnp
from jax import lax
from jax.experimental import pallas as pl
from jax.experimental.pallas import tpu as pltpu
from jax.sharding import PartitionSpec as P

EXPERTS = 8
CAP = 16
LANES = 128
VMEM_LIMIT = 63 * 1024 * 1024
BATCHES = ((0, 1, 4, 6), (2, 3, 5, 7))
LAG = 2
SEND_ORDER = (6, 4, 1, 3, 2)
LATER = (7, 5)
GROUPS = (2, 4)
RETURNS = ((1, 4, 6), (2, 3, 5, 7))
PLACE = {k: (b, i) for b, ks in enumerate(BATCHES) for i, k in enumerate(ks)}
BF16 = jnp.bfloat16
F32 = jnp.float32


def tile_of(size):
    for tile in (512, 256, 128):
        if size % tile == 0:
            return tile
    return size


def parts_of(table):
    high = table.astype(BF16).astype(F32)
    rest = table - high
    mid = rest.astype(BF16).astype(F32)
    low = (rest - mid).astype(BF16).astype(F32)
    return high, mid, low


def pick(table, members):
    reps = table.shape[1] // LANES
    rows = []
    for which in members:
        full = jnp.concatenate([which] * reps, axis=1)
        rows.append(jnp.take_along_axis(table, full, axis=0, mode="promise_in_bounds"))
    return jnp.concatenate(rows, axis=0)


def kernel(
    n,
    ids_hbm,
    mem_hbm,
    cw_hbm,
    tok_hbm,
    hidf_hbm,
    wg_hbm,
    wu_hbm,
    wd_hbm,
    inf_hbm,
    outf_hbm,
    o_ref,
    ids_ref,
    mem_ref,
    cw_ref,
    tok_ref,
    hidf_ref,
    wg,
    wu,
    wd,
    inf,
    outf,
    tab_hid,
    send,
    recv,
    who,
    weigh,
    gate_in,
    up_in,
    hidden,
    psend,
    precv,
    osend,
    home,
    placing,
    wsem,
    fsem,
    dsend,
    drecv,
    psems,
    precs,
    hsend,
    hrecv,
    xsend,
    xrecv,
):
    split = n // EXPERTS
    toks, width = tok_ref.shape
    units = wg.shape[1]
    seg = EXPERTS * CAP
    me = lax.axis_index("expert")
    own = lax.div(me, split)
    part = lax.rem(me, split)
    wide = tile_of(width)
    tile = tile_of(units)
    unit_tiles = units // tile
    out_tile = tile_of(width)
    tiles = width // out_tile
    ends = [[tiles * (g + 1) // n_g for g in range(n_g)] for n_g in GROUPS]
    batch_rows = recv.shape[0] // len(BATCHES)
    share_rows = batch_rows // split

    def expert_at(k):
        return lax.bitwise_xor(own, k)

    def part_at(j):
        return lax.rem(part + (j + split) % split, split)

    def far(k):
        return {"expert": expert_at(k) * split + part}

    def near(j):
        return {"expert": own * split + part_at(j)}

    def rows(index, count=CAP):
        return pl.ds(pl.multiple_of(index * count, count), count)

    barrier = pltpu.get_barrier_semaphore()
    for k in range(1, EXPERTS):
        pl.semaphore_signal(barrier, inc=1, device_id=far(k), device_id_type=pl.DeviceIdType.MESH)
    for j in range(1, split):
        pl.semaphore_signal(barrier, inc=1, device_id=near(j), device_id_type=pl.DeviceIdType.MESH)

    small = [
        pltpu.make_async_copy(src, dst, fsem.at[i])
        for i, (src, dst) in enumerate(
            ((ids_hbm, ids_ref), (mem_hbm, mem_ref), (cw_hbm, cw_ref), (tok_hbm, tok_ref))
        )
    ]
    loads = [
        pltpu.make_async_copy(inf_hbm.at[own], inf, fsem.at[4]),
        pltpu.make_async_copy(hidf_hbm, hidf_ref, fsem.at[5]),
        pltpu.make_async_copy(outf_hbm.at[own], outf, fsem.at[6]),
    ]

    def column_load(src, dst, size, t, sem):
        cols = pl.ds(t * size, size)
        return pltpu.make_async_copy(src.at[:, cols], dst.at[:, cols], sem)

    first = [
        [
            column_load(wg_hbm, wg, tile, t, wsem.at[0, t]),
            column_load(wu_hbm, wu, tile, t, wsem.at[1, t]),
        ]
        for t in range(unit_tiles)
    ]
    second = [column_load(wd_hbm, wd, out_tile, t, wsem.at[2, t]) for t in range(tiles)]
    for copy in small + loads:
        copy.start()
    for copy in sum(first, []) + second:
        copy.start(priority=1)

    down_i = lax.broadcasted_iota(jnp.int32, (toks, toks), 0)
    across = lax.broadcasted_iota(jnp.int32, (toks, toks), 1)

    def column(row):
        spread = jnp.broadcast_to(row.astype(F32), (toks, toks))
        return jnp.sum(jnp.where(across == down_i, spread, 0.0), axis=1, keepdims=True)

    lane = lax.broadcasted_iota(jnp.int32, (toks, seg), 1)
    lane_expert = lax.shift_right_logical(lane, CAP.bit_length() - 1)
    lane_slot = lax.bitwise_and(lane, CAP - 1)
    for copy in small[:3]:
        copy.wait()
    hit0 = column(ids_ref[0:1, :]) == lane_expert.astype(F32)
    hit1 = column(ids_ref[1:2, :]) == lane_expert.astype(F32)
    named = jnp.where(hit0 | hit1, 1.0, 0.0)
    earlier = jnp.where(across < down_i, 1.0, 0.0)
    rank = jnp.dot(earlier.astype(BF16), named.astype(BF16), preferred_element_type=F32)
    placed = jnp.where(rank == lane_slot.astype(F32), named, 0.0)
    placing[...] = placed.astype(BF16)
    member = column(mem_ref[...])
    col = lax.broadcasted_iota(jnp.int32, (toks, LANES), 1)

    def gather(which, data):
        return lax.dot_general(
            which.astype(BF16), data.astype(BF16), (((0,), (0,)), ((), ())), preferred_element_type=F32
        )

    meta_rows = jnp.zeros((seg, LANES), F32)
    for route, hit in ((0, hit0), (1, hit1)):
        meta = jnp.where(col == 0, member, 0.0)
        for spot, piece in enumerate(parts_of(column(cw_ref[route : route + 1, :]))):
            meta = jnp.where(col == 1 + spot, piece, meta)
        meta_rows = meta_rows + gather(jnp.where(hit, placed, 0.0), meta)
    send[:, width:] = meta_rows.astype(BF16)
    small[3].wait()
    for t in range(width // wide):
        cols = slice(t * wide, (t + 1) * wide)
        send[:, cols] = gather(placed, tok_ref[:, cols]).astype(BF16)

    pl.semaphore_wait(barrier, EXPERTS - 1 + split - 1)

    def landed(k, j):
        batch, slot = PLACE[k]
        each = len(BATCHES[batch])
        return rows(batch * split * each + part_at(-j) * each + slot)

    def direct(k):
        return pltpu.make_async_remote_copy(
            src_ref=send.at[rows(expert_at(k))],
            dst_ref=recv.at[landed(k, 0)],
            send_sem=dsend.at[k],
            recv_sem=drecv.at[k],
            device_id=far(k),
            device_id_type=pl.DeviceIdType.MESH,
        )

    def handed(k, j):
        return pltpu.make_async_remote_copy(
            src_ref=recv.at[landed(k, 0)] if k else send.at[rows(own)],
            dst_ref=recv.at[landed(k, 0)],
            send_sem=xsend.at[k, j],
            recv_sem=xrecv.at[k, j],
            device_id=near(j),
            device_id_type=pl.DeviceIdType.MESH,
        )

    for k in SEND_ORDER:
        direct(k).start()
    for j in range(1, split):
        handed(0, j).start()
    recv[landed(0, 0), :] = send[rows(own), :]

    for copy in loads:
        copy.wait()
    for g in range(2):
        for t in range(unit_tiles):
            cols = slice(t * tile, (t + 1) * tile)
            tab_hid[g, :, cols] = hidf_ref[:, g, cols]

    def hand_on(k):
        pltpu.make_async_remote_copy(
            src_ref=recv.at[landed(k, 0)],
            dst_ref=recv.at[landed(k, 0)],
            send_sem=dsend.at[k],
            recv_sem=drecv.at[k],
            device_id=far(k),
            device_id_type=pl.DeviceIdType.MESH,
        ).wait_recv()
        for j in range(1, split):
            handed(k, j).start()

    def got(k, j):
        pltpu.make_async_remote_copy(
            src_ref=recv.at[landed(k, j)],
            dst_ref=recv.at[landed(k, j)],
            send_sem=xsend.at[k, j],
            recv_sem=xrecv.at[k, j],
            device_id=near(j),
            device_id_type=pl.DeviceIdType.MESH,
        ).wait_recv()

    def scale_unit(k, j):
        mine = landed(k, j)
        meta = recv[mine, width:].astype(F32)
        which = jnp.broadcast_to(meta[:, 0:1], (CAP, LANES)).astype(jnp.int32)
        who[mine, :] = which
        if j == 0:
            batch, slot = PLACE[k]
            spot = lax.broadcasted_iota(jnp.int32, (CAP, LANES), 1)
            weight = jnp.sum(
                jnp.where((spot >= 1) & (spot < 4), meta, 0.0), axis=1, keepdims=True
            )
            weigh[batch, slot * CAP : (slot + 1) * CAP, :] = jnp.broadcast_to(weight, (CAP, LANES))
        members = [which[r : r + 8] for r in range(0, CAP, 8)]
        for t in range(width // wide):
            cols = slice(t * wide, (t + 1) * wide)
            data = recv[mine, cols].astype(F32)
            gate_in[mine, cols] = (data * pick(inf[:, cols], members)).astype(BF16)
            cols_up = slice(width + t * wide, width + (t + 1) * wide)
            up_in[mine, cols] = (data * pick(inf[:, cols_up], members)).astype(BF16)

    def hidden_units(b, low, high):
        mine = slice(b * batch_rows, (b + 1) * batch_rows)

        def hidden_tile(t, carry):
            cols = pl.ds(pl.multiple_of(t * tile, tile), tile)
            members = [
                who[b * batch_rows + r : b * batch_rows + r + 8, :] for r in range(0, batch_rows, 8)
            ]
            gate = jnp.dot(gate_in[mine, :], wg[:, cols], preferred_element_type=F32)
            gate = gate * pick(tab_hid[0, :, cols], members)
            up = jnp.dot(up_in[mine, :], wu[:, cols], preferred_element_type=F32)
            up = up * pick(tab_hid[1, :, cols], members)
            hidden[:, cols] = (gate / (1.0 + jnp.exp(-gate)) * up).astype(BF16)
            return carry

        lax.fori_loop(low, high, hidden_tile, 0, unroll=high - low)

    def share(b, t, j):
        return pltpu.make_async_remote_copy(
            src_ref=psend.at[b, t, rows(part_at(j), share_rows)],
            dst_ref=precv.at[b, t, j],
            send_sem=psems.at[b, t, j],
            recv_sem=precs.at[b, t, j],
            device_id=near(j),
            device_id_type=pl.DeviceIdType.MESH,
        )

    def back(g, k):
        batch, slot = PLACE[k]
        low = ends[batch][g - 1] if g else 0
        cols = pl.ds(low * out_tile, (ends[batch][g] - low) * out_tile)
        return pltpu.make_async_remote_copy(
            src_ref=osend.at[batch, pl.ds(slot * CAP, CAP), cols],
            dst_ref=home.at[rows(own), cols],
            send_sem=hsend.at[g, k],
            recv_sem=hrecv.at[g, k],
            device_id=far(k),
            device_id_type=pl.DeviceIdType.MESH,
        )

    def down_tile(b, t):
        cols = slice(t * out_tile, (t + 1) * out_tile)
        psend[b, t] = jnp.dot(hidden[...], wd[:, cols], preferred_element_type=F32).astype(BF16)
        for j in range(1, split):
            share(b, t, j).start()

    def finish(b, t):
        base = b * batch_rows + part * share_rows
        members = [
            who[pl.ds(pl.multiple_of(base + r, 8), 8), :] for r in range(0, share_rows, 8)
        ]
        total = psend[b, t, rows(part, share_rows), :].astype(F32)
        for j in range(1, split):
            share(b, t, j).wait_recv()
            total = total + precv[b, t, j].astype(F32)
        cols = slice(t * out_tile, (t + 1) * out_tile)
        weight = jnp.concatenate([weigh[b]] * (out_tile // LANES), axis=1)
        value = (total * pick(outf[:, cols], members) * weight).astype(BF16)
        osend[b, :, cols] = value
        if b == PLACE[0][0]:
            slot = PLACE[0][1]
            home[rows(own), cols] = value[slot * CAP : (slot + 1) * CAP]
        if t + 1 in ends[b]:
            for k in RETURNS[b]:
                back(ends[b].index(t + 1), k).start()

    half = (unit_tiles + 1) // 2
    ahead = max(0, tiles - LAG)

    scale_unit(0, 0)
    for k in BATCHES[0][1:]:
        hand_on(k)
        scale_unit(k, 0)
    for k in LATER:
        direct(k).start()
    for k in BATCHES[0]:
        for j in range(1, split):
            got(k, j)
            scale_unit(k, j)
    for copies in first[:half]:
        for copy in copies:
            copy.wait()
    hidden_units(0, 0, half)
    for copies in first[half:]:
        for copy in copies:
            copy.wait()
    for k in BATCHES[1][:2]:
        hand_on(k)
    hidden_units(0, half, unit_tiles)
    for t in range(tiles):
        second[t].wait()
        down_tile(0, t)
        if t >= LAG:
            finish(0, t - LAG)
        if t == min(2, tiles - 1):
            hand_on(BATCHES[1][2])
    hand_on(BATCHES[1][3])
    for k in BATCHES[1]:
        scale_unit(k, 0)
    for t in range(ahead, tiles):
        finish(0, t)
    for k in BATCHES[1]:
        for j in range(1, split):
            got(k, j)
            scale_unit(k, j)
    hidden_units(1, 0, unit_tiles)
    for t in range(tiles):
        down_tile(1, t)
        if t >= LAG:
            finish(1, t - LAG)
    for t in range(ahead, tiles):
        finish(1, t)

    for t in range(tiles):
        cols = slice(t * out_tile, (t + 1) * out_tile)
        for k in range(1, EXPERTS):
            stops = ends[PLACE[k][0]]
            for g, begin in enumerate([0] + stops[:-1]):
                if begin == t:
                    back(g, k).wait_recv()
        o_ref[:, cols] = jnp.dot(
            placing[...], home[:, cols], preferred_element_type=F32
        ).astype(BF16)

    for k in range(1, EXPERTS):
        direct(k).wait_send()
    for k in range(EXPERTS):
        for j in range(1, split):
            handed(k, j).wait_send()
    for t in range(tiles):
        for b in range(len(BATCHES)):
            for j in range(1, split):
                share(b, t, j).wait_send()
    for k in range(1, EXPERTS):
        for g in range(len(ends[PLACE[k][0]])):
            back(g, k).wait_send()


def per_device(
    tokens,
    expert_ids,
    member_ids,
    combine_weights,
    gate_weight,
    up_weight,
    down_weight,
    input_factors,
    hidden_factors,
    output_factors,
):
    n = lax.axis_size("expert")
    split = n // EXPERTS
    toks, width = tokens.shape
    units = gate_weight.shape[1]
    members = input_factors.shape[1]
    seg = EXPERTS * CAP
    all_rows = n * CAP
    batches = len(BATCHES)
    batch_rows = all_rows // batches
    out_tile = tile_of(width)
    tiles = width // out_tile
    unit_tiles = units // tile_of(units)
    vmem = pl.BlockSpec(memory_space=pltpu.VMEM)
    hbm = pl.BlockSpec(memory_space=pl.ANY)
    dma = pltpu.SemaphoreType.DMA
    return pl.pallas_call(
        functools.partial(kernel, n),
        out_shape=pltpu.VMEM((toks, width), BF16),
        in_specs=[hbm] * 10,
        out_specs=vmem,
        scratch_shapes=[
            pltpu.VMEM((2, toks), jnp.int32),
            pltpu.VMEM((1, toks), jnp.int32),
            pltpu.VMEM((2, toks), F32),
            pltpu.VMEM((toks, width), BF16),
            pltpu.VMEM(hidden_factors.shape, F32),
            pltpu.VMEM((width, units), BF16),
            pltpu.VMEM((width, units), BF16),
            pltpu.VMEM((units, width), BF16),
            pltpu.VMEM((members, 2 * width), F32),
            pltpu.VMEM((members, width), F32),
            pltpu.VMEM((2, members, units), F32),
            pltpu.VMEM((seg, width + LANES), BF16),
            pltpu.VMEM((all_rows, width + LANES), BF16),
            pltpu.VMEM((all_rows, LANES), jnp.int32),
            pltpu.VMEM((batches, seg // batches, LANES), F32),
            pltpu.VMEM((all_rows, width), BF16),
            pltpu.VMEM((all_rows, width), BF16),
            pltpu.VMEM((batch_rows, units), BF16),
            pltpu.VMEM((batches, tiles, batch_rows, out_tile), BF16),
            pltpu.VMEM((batches, tiles, split, seg // batches, out_tile), BF16),
            pltpu.VMEM((batches, seg // batches, width), BF16),
            pltpu.VMEM((seg, width), BF16),
            pltpu.VMEM((toks, seg), BF16),
            dma((3, max(unit_tiles, tiles))),
            dma((7,)),
            dma((EXPERTS,)),
            dma((EXPERTS,)),
            dma((batches, tiles, split)),
            dma((batches, tiles, split)),
            dma((tiles, EXPERTS)),
            dma((tiles, EXPERTS)),
            dma((EXPERTS, split)),
            dma((EXPERTS, split)),
        ],
        compiler_params=pltpu.CompilerParams(
            collective_id=0, has_side_effects=True, vmem_limit_bytes=VMEM_LIMIT
        ),
        name="moe_step",
    )(
        expert_ids.T,
        member_ids.reshape(1, toks),
        combine_weights.T,
        tokens,
        hidden_factors,
        gate_weight,
        up_weight,
        down_weight,
        input_factors,
        output_factors,
    )


def solution(mesh):
    in_specs = (
        P(("groups", "expert"), None),
        P(("groups", "expert"), None),
        P(("groups", "expert")),
        P(("groups", "expert"), None),
        P(None, "expert"),
        P(None, "expert"),
        P("expert", None),
        P(),
        P(None, None, "expert"),
        P(),
    )
    out_specs = P(("groups", "expert"), None)
    return jax.shard_map(
        per_device, mesh=mesh, in_specs=in_specs, out_specs=out_specs, check_vma=False
    )
```
